32 devices in a mesh: gz: 8 (over z, y), gy: 4 (over x, core).
Axes of the slice: x: 2, y: 2, z: 4, core: 2. Of those that a mesh axis runs over, the one named last changes fastest.
Arguments:
- orbitals: bfloat16 [96, 96, 96, 256], P('gz', 'gy'), may hold values from -6 to 6
- pair_list: int32 [64, 2], replicated, may hold values from 0 to 255
- box_anchor: int32 [256, 3], replicated, may hold values from 0 to 95
- pair_live: int32 [64], replicated, may hold values from 0 to 1, as said below
Outputs:
- gradient: float32 [96, 96, 96, 256], P('gz', 'gy')
The draws below stay inside these ranges and needn't reach their ends.
Inputs may be any that keep to these rules, and one draw needn't show every extreme that they name: `pair_live`: in each owner's block of 2 slots the live slots come first; at least one slot of every block is live, some block has all 2 live, and some other block has exactly one live.
All inputs are finite; a program needn't handle non-finite values.
Results may differ from the reference program's by a relative error of at most 0.0035.
Values may be sent and summed in bfloat16 or wider, within the bound.
A program may use at most 192 MiB of HBM per device.

```python
import jax
import jax.numpy as jnp
from jax import lax

ORB = 256
GRID = 96
B = 64
PAIR_DEV = 2
PAIRS = 64


def draw_pair_live(key, part):
    base = jax.random.fold_in(key, 7)
    first_key, second_key, third_key = jax.random.split(base, 3)
    owners = PAIRS // PAIR_DEV
    counts = jax.random.randint(first_key, (owners,), 1, PAIR_DEV + 1)
    fullest = jax.random.randint(second_key, (), 0, owners)
    offset = jax.random.randint(third_key, (), 1, owners)
    sparsest = (fullest + offset) % owners
    counts = jnp.where(jnp.arange(owners) == fullest, PAIR_DEV, counts)
    counts = jnp.where(jnp.arange(owners) == sparsest, 1, counts)
    slot = jnp.arange(PAIRS) % PAIR_DEV
    return (slot < jnp.repeat(counts, PAIR_DEV)).astype(jnp.int32)


def place_ends(values, key, smallest, high):
    longest = values.shape.index(max(values.shape))
    spots = []
    for shift in (0, 1):
        where = [jax.random.randint(jax.random.fold_in(key, axis), (), 0, length) for axis, length in enumerate(values.shape)]
        where[longest] = (where[longest] + shift) % values.shape[longest]
        spots.append(tuple(where))
    return values.at[spots[0]].set(smallest).at[spots[1]].set(high)


def steps_of(rng, shape, pieces, least, largest):
    def one(axis_at, shards_of):
        steps = jax.random.uniform(jax.random.fold_in(jax.random.fold_in(rng, 6), axis_at), (shards_of,), jnp.float32, least / len(pieces), largest / len(pieces))
        return jnp.repeat(jnp.exp(steps), shape[axis_at] // shards_of).reshape((-1,) + (1,) * (len(shape) - axis_at - 1))

    gain = one(*pieces[0])
    for cut in pieces[1:]:
        gain = gain * one(*cut)
    return gain


def centred(key, dims, scale, limit, shards=(), held_as=jnp.bfloat16):
    gain = steps_of(key, dims, shards, -0.22, 0.18) if shards else 1.0
    values = jax.random.normal(key, dims, jnp.float32) * scale * gain
    return jnp.minimum(jnp.maximum(values, -limit), limit).astype(held_as)


def setup_inputs(seed: int = 0) -> dict:
    key_of = jax.random.split(jax.random.key(seed), 5)
    return {
        "orbitals": centred(key_of[0], (GRID, GRID, GRID, ORB), 1.0, 6.0, ((0, 8), (1, 4))),
        "pair_list": place_ends(jax.random.randint(key_of[1], (PAIRS, 2), 0, ORB), jax.random.fold_in(key_of[1], 1), 0, ORB - 1).astype(jnp.int32),
        "box_anchor": place_ends(jax.random.randint(key_of[2], (ORB, 3), 0, GRID), jax.random.fold_in(key_of[2], 1), 0, GRID - 1).astype(jnp.int32),
        "pair_live": draw_pair_live(jax.random.fold_in(key_of[4], 71), 0),
    }


def poisson_box(density):
    side = density.shape[-1]
    index = jnp.arange(1, side + 1).astype(jnp.float32)
    table = jnp.sqrt(2.0 / (side + 1.0)) * jnp.sin(jnp.pi * index[:, None] * index[None, :] / (side + 1.0))
    eigen = 2.0 - 2.0 * jnp.cos(jnp.pi * index / (side + 1.0))
    denom = eigen[:, None, None] + eigen[None, :, None] + eigen[None, None, :]
    hp = lax.Precision.HIGHEST

    def apply_all(field):
        field = jnp.einsum('...abc,ai->...ibc', field, table, precision=hp)
        field = jnp.einsum('...ibc,bj->...ijc', field, table, precision=hp)
        return jnp.einsum('...ijc,ck->...ijk', field, table, precision=hp)
    return apply_all(apply_all(density) / denom)

def shift_grid(grid, anchor, sign):
    grid = jnp.roll(grid, sign * anchor[0], axis=0)
    grid = jnp.roll(grid, sign * anchor[1], axis=1)
    return jnp.roll(grid, sign * anchor[2], axis=2)

def reference(orbitals, pair_list, box_anchor, pair_live):
    major = jnp.transpose(orbitals, (3, 0, 1, 2))
    side = B

    def one_pair(p, carry):
        first = pair_list[p, 0]
        second = pair_list[p, 1]
        anchor = box_anchor[first]
        left = shift_grid(major[first], anchor, -1)[:side, :side, :side]
        right = shift_grid(major[second], anchor, -1)[:side, :side, :side]
        density = left.astype(jnp.float32) * right.astype(jnp.float32)
        potential = poisson_box(density)
        live = pair_live[p].astype(jnp.float32)
        term = (potential * right.astype(jnp.float32) * live).astype(jnp.bfloat16)
        padded = jnp.pad(term, ((0, GRID - side), (0, GRID - side), (0, GRID - side)))
        placed = shift_grid(padded, anchor, 1).astype(jnp.float32)
        return carry.at[first].add(placed)
    start = jnp.zeros((ORB, GRID, GRID, GRID), jnp.float32)
    action_major = lax.fori_loop(0, PAIRS, one_pair, start)
    action = jnp.transpose(action_major, (1, 2, 3, 0)).reshape(-1, ORB)
    action_low = action.astype(jnp.bfloat16)
    flat = orbitals.reshape(-1, ORB)
    tiles = lax.dot_general(flat, action_low, (((0,), (0,)), ((), ())), preferred_element_type=jnp.float32)
    tiles = (tiles / (float(B) ** 3 / 4.0)).astype(jnp.bfloat16)
    gradient = action - jnp.dot(flat, tiles, preferred_element_type=jnp.float32)
    return gradient.reshape(GRID, GRID, GRID, ORB)
```

```python
import functools

import jax
import jax.numpy as jnp
import numpy as np
from jax import lax
from jax.experimental import pallas as pl
from jax.experimental.pallas import tpu as pltpu
from jax.sharding import PartitionSpec as P

B = 64
LANES = 128
BF = jnp.bfloat16
F32 = jnp.float32
VMEM_LIMIT = 56 * 1024 * 1024


def dot_nt(a, b):
    return lax.dot_general(a, b, (((1,), (1,)), ((), ())), preferred_element_type=F32)


def dot_nn(a, b):
    return lax.dot_general(a, b, (((1,), (0,)), ((), ())), preferred_element_type=F32)


def dot_tn(a, b):
    return lax.dot_general(a, b, (((0,), (0,)), ((), ())), preferred_element_type=F32)


def split(a):
    hi = a.astype(BF)
    return hi, (a - hi.astype(F32)).astype(BF)


def density_kernel(per_dev, ax_ref, onehot_ref, orb_ref, out_ref, scr):
    _, rows, across, _ = orb_ref.shape
    pairs = onehot_ref.shape[0] // 2
    owners = pairs // per_dev

    def row(y, _):
        both = dot_nt(onehot_ref[...], orb_ref[0, y])
        scr[pl.ds(pl.multiple_of(y * pairs, 8), pairs), :across] = both[:pairs] * both[pairs:]
        return 0

    lax.fori_loop(0, rows, row, 0, unroll=4)
    lane = lax.broadcasted_iota(jnp.int32, (rows, LANES), 1)

    def owner(d, _):
        acc = jnp.zeros((rows, LANES), F32)
        for s in range(per_dev):
            p = d * per_dev + s
            a = ax_ref[p]
            base = s * B
            x = scr[pl.ds(p, rows, stride=pairs), :]
            near = pltpu.roll(x, lax.rem(base - a + 2 * LANES, LANES), 1)
            far = pltpu.roll(x, lax.rem(base + across - a + 2 * LANES, LANES), 1)
            rel = lane - base
            acc = jnp.where((rel >= 0) & (rel < B), jnp.where(rel < across - a, near, far), acc)
        out_ref[d, 0] = acc.astype(BF)
        return 0

    lax.fori_loop(0, owners, owner, 0, unroll=4)


def poisson_kernel(per_dev, extent, az_ref, ay_ref, ly_ref, left_ref, sx2_ref, sx3_ref, lzx_ref, in_ref, out_ref, field, ring):
    n_gz, n_gy, depth, rows, _ = in_ref.shape
    lane = lax.broadcasted_iota(jnp.int32, (B, LANES), 1)
    lane_all = lax.broadcasted_iota(jnp.int32, (extent, LANES), 1)
    slots = ring.shape[0]

    def along_rows(e):
        hi, lo = split(e)
        return dot_nn(left_ref[...], jnp.concatenate([hi, hi, lo], axis=0))

    def cut(a, slot):
        out = None
        for s in range(per_dev):
            z = lax.rem(az_ref[s] + a, extent)
            gz = z // depth
            zi = z - gz * depth
            for gy in range(n_gy):
                part = in_ref[gz, gy, zi].astype(F32)
                ring[slot, s, gy * rows:(gy + 1) * rows] = part
                ring[slot, s, extent + gy * rows:extent + (gy + 1) * rows] = part
            got = ring[slot, s, pl.ds(ay_ref[s], B), :]
            out = got if out is None else jnp.where(lane >= s * B, got, out)
        return out

    def first(step, _):
        for slot in range(slots):
            a = step * slots + slot
            d = cut(a, slot).astype(BF)
            e = dot_nn(jnp.concatenate([d, d], axis=1), sx2_ref[...])
            field[pl.ds(pl.multiple_of(a * B, 8), B), :] = along_rows(e)
        return 0

    lax.fori_loop(0, B // slots, first, 0)

    def middle(step, _):
        for k in range(4):
            y = step * 4 + k
            e = along_rows(field[pl.ds(y, B, stride=B), :])
            e = e / (lzx_ref[...] + ly_ref[y])
            field[pl.ds(y, B, stride=B), :] = along_rows(e)
        return 0

    lax.fori_loop(0, B // 4, middle, 0)

    def last(step, _):
        for k in range(4):
            a = step * 4 + k
            at = pl.ds(pl.multiple_of(a * B, 8), B)
            hi, lo = split(along_rows(field[at, :]))
            field[at, :] = dot_nn(jnp.concatenate([hi, hi, lo], axis=1), sx3_ref[...])
        return 0

    lax.fori_loop(0, B // 4, last, 0)
    ring[...] = jnp.zeros_like(ring)

    def place(step, _):
        for slot in range(slots):
            z = step * slots + slot
            out = jnp.zeros((extent, LANES), F32)
            for s in range(per_dev):
                a = lax.rem(z - az_ref[s] + extent, extent)
                v = field[pl.ds(pl.multiple_of(jnp.minimum(a, B - 1) * B, 8), B), :]
                v = jnp.where(a < B, v, 0.0)
                ring[slot, s, :B] = v
                ring[slot, s, extent:extent + B] = v
                got = ring[slot, s, pl.ds(extent - ay_ref[s], extent), :]
                out = jnp.where(lane_all >= s * B, got, out)
            gz = z // depth
            zi = z - gz * depth
            for gy in range(n_gy):
                out_ref[gz, gy, zi] = out[gy * rows:(gy + 1) * rows].astype(BF)
        return 0

    lax.fori_loop(0, extent // slots, place, 0)


def term_kernel(per_dev, ax_ref, live_ref, onehot_ref, same_ref, orb_ref, in_ref, term_ref, tile_ref, scr):
    _, rows, across, _ = orb_ref.shape
    pairs = onehot_ref.shape[0]
    owners = pairs // per_dev
    lane = lax.broadcasted_iota(jnp.int32, (rows, LANES), 1)

    def owner(d, _):
        v = in_ref[d, 0].astype(F32)
        for s in range(per_dev):
            p = d * per_dev + s
            a = ax_ref[p]
            base = s * B
            near = pltpu.roll(v, lax.rem(a - base + 2 * LANES, LANES), 1)
            far = pltpu.roll(v, lax.rem(a - across - base + 3 * LANES, LANES), 1)
            rel = lane - a
            lit = live_ref[p] > 0
            v_p = jnp.where((rel >= 0) & (rel < B) & lit, near, 0.0)
            v_p = jnp.where((rel + across < B) & lit, far, v_p)
            scr[pl.ds(p, rows, stride=pairs), :] = v_p
        return 0

    lax.fori_loop(0, owners, owner, 0, unroll=4)

    @pl.when(pl.program_id(0) == 0)
    def _():
        tile_ref[...] = jnp.zeros_like(tile_ref)

    step = 4 if rows % 4 == 0 else 1

    def row(i, acc):
        for k in range(step):
            y = i * step + k
            o = orb_ref[0, y]
            psi = dot_nt(onehot_ref[...], o)
            t = (scr[pl.ds(pl.multiple_of(y * pairs, 8), pairs), :across] * psi).astype(BF)
            term_ref[0, y] = t
            low = dot_nn(same_ref[...], t).astype(BF)
            acc = acc + dot_nn(low, o)
        return acc

    tile_ref[...] += lax.fori_loop(0, rows // step, row, jnp.zeros(tile_ref.shape, F32))


def gradient_kernel(sel_ref, tiles_ref, orb_ref, term_ref, out_ref):
    _, rows, _, _ = orb_ref.shape

    def row(y, _):
        out_ref[0, y] = dot_tn(term_ref[0, y], sel_ref[...]) - dot_nn(orb_ref[0, y], tiles_ref[...])
        return 0

    lax.fori_loop(0, rows, row, 0, unroll=4)


def tables(per_dev):
    index = np.arange(1, B + 1, dtype=np.float64)
    s = np.sqrt(2.0 / (B + 1.0)) * np.sin(np.pi * index[:, None] * index[None, :] / (B + 1.0))
    eigen = 2.0 - 2.0 * np.cos(np.pi * index / (B + 1.0))
    hi = s.astype(jnp.bfloat16)
    lo = (s - hi.astype(np.float64)).astype(jnp.bfloat16)
    eye = np.eye(per_dev)
    bd = lambda m: np.kron(eye, m.astype(np.float32)).astype(jnp.bfloat16)
    left = np.concatenate([hi, lo, hi], axis=1)
    sx2 = np.concatenate([bd(hi), bd(lo)], axis=0)
    sx3 = np.concatenate([bd(hi), bd(lo), bd(hi)], axis=0)
    lzx = (eigen[:, None] + np.tile(eigen, per_dev)[None, :]).astype(np.float32)
    return eigen.astype(np.float32), left, sx2, sx3, lzx


def body(orbitals, pair_list, box_anchor, pair_live):
    depth, rows, across, norb = orbitals.shape
    n_gz = lax.axis_size("gz")
    n_gy = lax.axis_size("gy")
    owners = n_gz * n_gy
    pairs = pair_list.shape[0]
    per_dev = pairs // owners
    extent = depth * n_gz
    firsts = pair_list[:, 0]
    seconds = pair_list[:, 1]
    anchors = box_anchor[firsts]
    ax = anchors[:, 2]
    me = lax.axis_index(("gz", "gy"))
    mine = lax.dynamic_slice_in_dim(anchors, me * per_dev, per_dev, 0)
    orbs = jnp.arange(norb)
    sel = firsts[:, None] == orbs[None, :]
    hot_first = sel.astype(BF)
    hot_second = (seconds[:, None] == orbs[None, :]).astype(BF)
    hot_both = jnp.concatenate([hot_first, hot_second], axis=0)
    equal = firsts[:, None] == firsts[None, :]
    same = equal.astype(BF)
    slot = jnp.arange(pairs)
    leads = jnp.logical_not(jnp.any(equal & (slot[None, :] < slot[:, None]), axis=1))
    lead_sel = (sel & leads[:, None]).astype(BF)

    smem = pl.BlockSpec(memory_space=pltpu.SMEM)
    full = lambda shape: pl.BlockSpec(shape, lambda z: (0,) * len(shape))
    orb_spec = pl.BlockSpec((1, rows, across, norb), lambda z: (z, 0, 0, 0))
    slab_spec = pl.BlockSpec((owners, 1, rows, LANES), lambda z: (0, z, 0, 0))
    slab = jax.ShapeDtypeStruct((owners, depth, rows, LANES), BF)
    params = pltpu.CompilerParams(dimension_semantics=("arbitrary",), vmem_limit_bytes=VMEM_LIMIT)

    density = pl.pallas_call(
        functools.partial(density_kernel, per_dev),
        grid=(depth,),
        out_shape=slab,
        in_specs=[smem, full((2 * pairs, norb)), orb_spec],
        out_specs=slab_spec,
        scratch_shapes=[pltpu.VMEM((rows * pairs, LANES), F32)],
        compiler_params=params,
        name="density",
    )(ax, hot_both, orbitals)
    incoming = lax.all_to_all(density, ("gz", "gy"), split_axis=0, concat_axis=0, tiled=True)
    incoming = incoming.reshape(n_gz, n_gy, depth, rows, LANES)

    eigen, left, sx2, sx3, lzx = tables(per_dev)
    vmem = pl.BlockSpec(memory_space=pltpu.VMEM)
    potential = pl.pallas_call(
        functools.partial(poisson_kernel, per_dev, extent),
        out_shape=jax.ShapeDtypeStruct(incoming.shape, BF),
        in_specs=[smem, smem, smem, vmem, vmem, vmem, vmem, vmem],
        out_specs=vmem,
        scratch_shapes=[
            pltpu.VMEM((B * B, LANES), F32),
            pltpu.VMEM((4, per_dev, 2 * extent, LANES), F32),
        ],
        compiler_params=pltpu.CompilerParams(vmem_limit_bytes=VMEM_LIMIT),
        name="poisson",
    )(mine[:, 0], mine[:, 1], jnp.asarray(eigen), jnp.asarray(left), jnp.asarray(sx2), jnp.asarray(sx3), jnp.asarray(lzx), incoming)
    back = lax.all_to_all(potential.reshape(owners, depth, rows, LANES), ("gz", "gy"), split_axis=0, concat_axis=0, tiled=True)

    term, part = pl.pallas_call(
        functools.partial(term_kernel, per_dev),
        grid=(depth,),
        out_shape=(
            jax.ShapeDtypeStruct((depth, rows, pairs, across), BF),
            jax.ShapeDtypeStruct((pairs, norb), F32),
        ),
        in_specs=[smem, smem, full((pairs, norb)), full((pairs, pairs)), orb_spec, slab_spec],
        out_specs=(
            pl.BlockSpec((1, rows, pairs, across), lambda z: (z, 0, 0, 0)),
            full((pairs, norb)),
        ),
        scratch_shapes=[pltpu.VMEM((rows * pairs, LANES), F32)],
        compiler_params=params,
        name="term",
    )(ax, pair_live, hot_second, same, orbitals, back)
    summed = lax.psum(part, ("gz", "gy"))
    rows_of = (summed / (float(B) ** 3 / 4.0)).astype(BF)
    tiles = dot_tn(rows_of, lead_sel).astype(BF)

    return pl.pallas_call(
        gradient_kernel,
        grid=(depth,),
        out_shape=jax.ShapeDtypeStruct(orbitals.shape, F32),
        in_specs=[
            full((pairs, norb)),
            full((norb, norb)),
            orb_spec,
            pl.BlockSpec((1, rows, pairs, across), lambda z: (z, 0, 0, 0)),
        ],
        out_specs=orb_spec,
        compiler_params=params,
        name="gradient",
    )(hot_first, tiles, orbitals, term)


def solution(mesh):
    return jax.shard_map(
        body,
        mesh=mesh,
        in_specs=(P("gz", "gy", None, None), P(), P(), P()),
        out_specs=P("gz", "gy", None, None),
        check_vma=False,
    )
```

```python
import functools

import jax
import jax.numpy as jnp
import numpy as np
from jax import lax
from jax.experimental import pallas as pl
from jax.experimental.pallas import tpu as pltpu
from jax.sharding import PartitionSpec as P

B = 64
LANES = 128
GAP = 8
BF = jnp.bfloat16
F32 = jnp.float32
VMEM_LIMIT = 56 * 1024 * 1024


def dot_nt(a, b):
    return lax.dot_general(a, b, (((1,), (1,)), ((), ())), preferred_element_type=F32)


def dot_nn(a, b):
    return lax.dot_general(a, b, (((1,), (0,)), ((), ())), preferred_element_type=F32)


def dot_tn(a, b):
    return lax.dot_general(a, b, (((0,), (0,)), ((), ())), preferred_element_type=F32)


def split(a):
    hi = a.astype(BF)
    return hi, (a - hi.astype(F32)).astype(BF)


def density_kernel(per_dev, ax_ref, onehot_ref, orb_ref, out_ref, psi_ref, scr):
    _, rows, across, _ = orb_ref.shape
    pairs = onehot_ref.shape[0] // 2
    pitch = pairs + GAP
    owners = pairs // per_dev

    def row(y, _):
        both = dot_nt(onehot_ref[...], orb_ref[0, y])
        scr[pl.ds(pl.multiple_of(y * pitch, 8), pairs), :across] = both[:pairs] * both[pairs:]
        psi_ref[0, y] = both[pairs:].astype(BF)
        return 0

    lax.fori_loop(0, rows, row, 0, unroll=4)
    lane = lax.broadcasted_iota(jnp.int32, (rows, LANES), 1)

    def owner(d, _):
        acc = jnp.zeros((rows, LANES), F32)
        for s in range(per_dev):
            p = d * per_dev + s
            a = ax_ref[p]
            base = s * B
            x = scr[pl.ds(p, rows, stride=pitch), :]
            near = pltpu.roll(x, lax.rem(base - a + 2 * LANES, LANES), 1)
            far = pltpu.roll(x, lax.rem(base + across - a + 2 * LANES, LANES), 1)
            rel = lane - base
            acc = jnp.where((rel >= 0) & (rel < B), jnp.where(rel < across - a, near, far), acc)
        out_ref[d, 0] = acc.astype(BF)
        return 0

    lax.fori_loop(0, owners, owner, 0, unroll=4)


def poisson_kernel(per_dev, extent, az_ref, ay_ref, ly_ref, left_ref, sx2_ref, sx3_ref, lzx_ref, in_ref, out_ref, field, ring):
    n_gz, n_gy, depth, rows, _ = in_ref.shape
    lane = lax.broadcasted_iota(jnp.int32, (B, LANES), 1)
    lane_all = lax.broadcasted_iota(jnp.int32, (extent, LANES), 1)
    slots = ring.shape[0]
    pitch = B + GAP

    def along_rows(e):
        hi, lo = split(e)
        return dot_nn(left_ref[...], jnp.concatenate([hi, hi, lo], axis=0))

    def cut(a, slot):
        out = None
        for s in range(per_dev):
            z = lax.rem(az_ref[s] + a, extent)
            gz = z // depth
            zi = z - gz * depth
            for gy in range(n_gy):
                part = in_ref[gz, gy, zi].astype(F32)
                ring[slot, s, gy * rows:(gy + 1) * rows] = part
                ring[slot, s, extent + gy * rows:extent + (gy + 1) * rows] = part
            got = ring[slot, s, pl.ds(ay_ref[s], B), :]
            out = got if out is None else jnp.where(lane >= s * B, got, out)
        return out

    def first(step, _):
        for slot in range(slots):
            a = step * slots + slot
            d = cut(a, slot).astype(BF)
            e = dot_nn(jnp.concatenate([d, d], axis=1), sx2_ref[...])
            field[pl.ds(pl.multiple_of(a * pitch, 8), B), :] = along_rows(e)
        return 0

    lax.fori_loop(0, B // slots, first, 0)

    def middle(step, _):
        for k in range(4):
            y = step * 4 + k
            e = along_rows(field[pl.ds(y, B, stride=pitch), :])
            e = e / (lzx_ref[...] + ly_ref[y])
            field[pl.ds(y, B, stride=pitch), :] = along_rows(e)
        return 0

    lax.fori_loop(0, B // 4, middle, 0)

    def last(step, _):
        for k in range(4):
            a = step * 4 + k
            at = pl.ds(pl.multiple_of(a * pitch, 8), B)
            hi, lo = split(along_rows(field[at, :]))
            field[at, :] = dot_nn(jnp.concatenate([hi, hi, lo], axis=1), sx3_ref[...])
        return 0

    lax.fori_loop(0, B // 4, last, 0)
    ring[...] = jnp.zeros_like(ring)

    def place(step, _):
        for slot in range(slots):
            z = step * slots + slot
            out = jnp.zeros((extent, LANES), F32)
            for s in range(per_dev):
                a = lax.rem(z - az_ref[s] + extent, extent)
                v = field[pl.ds(pl.multiple_of(jnp.minimum(a, B - 1) * pitch, 8), B), :]
                v = jnp.where(a < B, v, 0.0)
                ring[slot, s, :B] = v
                ring[slot, s, extent:extent + B] = v
                got = ring[slot, s, pl.ds(extent - ay_ref[s], extent), :]
                out = jnp.where(lane_all >= s * B, got, out)
            gz = z // depth
            zi = z - gz * depth
            for gy in range(n_gy):
                out_ref[gz, gy, zi] = out[gy * rows:(gy + 1) * rows].astype(BF)
        return 0

    lax.fori_loop(0, extent // slots, place, 0)


def term_kernel(per_dev, ax_ref, live_ref, psi_ref, orb_ref, in_ref, term_ref, tile_ref, scr):
    _, rows, across, _ = orb_ref.shape
    pairs = psi_ref.shape[2]
    pitch = pairs + GAP
    owners = pairs // per_dev
    lane = lax.broadcasted_iota(jnp.int32, (rows, LANES), 1)

    def owner(d, _):
        v = in_ref[d, 0].astype(F32)
        for s in range(per_dev):
            p = d * per_dev + s
            a = ax_ref[p]
            base = s * B
            near = pltpu.roll(v, lax.rem(a - base + 2 * LANES, LANES), 1)
            far = pltpu.roll(v, lax.rem(a - across - base + 3 * LANES, LANES), 1)
            rel = lane - a
            lit = live_ref[p] > 0
            v_p = jnp.where((rel >= 0) & (rel < B) & lit, near, 0.0)
            v_p = jnp.where((rel + across < B) & lit, far, v_p)
            scr[pl.ds(p, rows, stride=pitch), :] = v_p
        return 0

    lax.fori_loop(0, owners, owner, 0, unroll=4)

    @pl.when(pl.program_id(0) == 0)
    def _():
        tile_ref[...] = jnp.zeros_like(tile_ref)

    step = 4 if rows % 4 == 0 else 1

    def row(i, acc):
        for k in range(step):
            y = i * step + k
            v = scr[pl.ds(pl.multiple_of(y * pitch, 8), pairs), :across]
            t = (v * psi_ref[0, y].astype(F32)).astype(BF)
            term_ref[0, y] = t
            acc = acc + dot_nn(t, orb_ref[0, y])
        return acc

    tile_ref[...] += lax.fori_loop(0, rows // step, row, jnp.zeros(tile_ref.shape, F32))


def gradient_kernel(sel_ref, tiles_ref, orb_ref, term_ref, out_ref):
    _, rows, across, norb = orb_ref.shape
    step = 4 if rows % 4 == 0 else 1

    def some(i, _):
        at = pl.ds(i * step, step)
        o = orb_ref[0, at].reshape(step * across, norb)
        c = jnp.concatenate([term_ref[0, i * step + k].T for k in range(step)], axis=0)
        total = dot_nn(c, sel_ref[...]) - dot_nn(o, tiles_ref[...])
        out_ref[0, at] = total.reshape(step, across, norb)
        return 0

    lax.fori_loop(0, rows // step, some, 0, unroll=2)


def tables(per_dev):
    index = np.arange(1, B + 1, dtype=np.float64)
    s = np.sqrt(2.0 / (B + 1.0)) * np.sin(np.pi * index[:, None] * index[None, :] / (B + 1.0))
    eigen = 2.0 - 2.0 * np.cos(np.pi * index / (B + 1.0))
    hi = s.astype(jnp.bfloat16)
    lo = (s - hi.astype(np.float64)).astype(jnp.bfloat16)
    eye = np.eye(per_dev)
    bd = lambda m: np.kron(eye, m.astype(np.float32)).astype(jnp.bfloat16)
    left = np.concatenate([hi, lo, hi], axis=1)
    sx2 = np.concatenate([bd(hi), bd(lo)], axis=0)
    sx3 = np.concatenate([bd(hi), bd(lo), bd(hi)], axis=0)
    lzx = (eigen[:, None] + np.tile(eigen, per_dev)[None, :]).astype(np.float32)
    return eigen.astype(np.float32), left, sx2, sx3, lzx


def body(orbitals, pair_list, box_anchor, pair_live):
    depth, rows, across, norb = orbitals.shape
    n_gz = lax.axis_size("gz")
    n_gy = lax.axis_size("gy")
    owners = n_gz * n_gy
    pairs = pair_list.shape[0]
    per_dev = pairs // owners
    extent = depth * n_gz
    firsts = pair_list[:, 0]
    seconds = pair_list[:, 1]
    anchors = box_anchor[firsts]
    ax = anchors[:, 2]
    me = lax.axis_index(("gz", "gy"))
    mine = lax.dynamic_slice_in_dim(anchors, me * per_dev, per_dev, 0)
    orbs = jnp.arange(norb)
    sel = firsts[:, None] == orbs[None, :]
    hot_first = sel.astype(BF)
    hot_second = (seconds[:, None] == orbs[None, :]).astype(BF)
    hot_both = jnp.concatenate([hot_first, hot_second], axis=0)

    smem = pl.BlockSpec(memory_space=pltpu.SMEM)
    full = lambda shape: pl.BlockSpec(shape, lambda z: (0,) * len(shape))
    orb_spec = pl.BlockSpec((1, rows, across, norb), lambda z: (z, 0, 0, 0))
    slab_spec = pl.BlockSpec((owners, 1, rows, LANES), lambda z: (0, z, 0, 0))
    plane_spec = pl.BlockSpec((1, rows, pairs, across), lambda z: (z, 0, 0, 0))
    slab = jax.ShapeDtypeStruct((owners, depth, rows, LANES), BF)
    params = pltpu.CompilerParams(dimension_semantics=("arbitrary",), vmem_limit_bytes=VMEM_LIMIT)

    density, psi = pl.pallas_call(
        functools.partial(density_kernel, per_dev),
        grid=(depth,),
        out_shape=(slab, jax.ShapeDtypeStruct((depth, rows, pairs, across), BF)),
        in_specs=[smem, full((2 * pairs, norb)), orb_spec],
        out_specs=(slab_spec, plane_spec),
        scratch_shapes=[pltpu.VMEM((rows * (pairs + GAP), LANES), F32)],
        compiler_params=params,
        name="density",
    )(ax, hot_both, orbitals)
    incoming = lax.all_to_all(density, ("gz", "gy"), split_axis=0, concat_axis=0, tiled=True)
    incoming = incoming.reshape(n_gz, n_gy, depth, rows, LANES)

    eigen, left, sx2, sx3, lzx = tables(per_dev)
    vmem = pl.BlockSpec(memory_space=pltpu.VMEM)
    potential = pl.pallas_call(
        functools.partial(poisson_kernel, per_dev, extent),
        out_shape=jax.ShapeDtypeStruct(incoming.shape, BF),
        in_specs=[smem, smem, smem, vmem, vmem, vmem, vmem, vmem],
        out_specs=vmem,
        scratch_shapes=[
            pltpu.VMEM((B * (B + GAP), LANES), F32),
            pltpu.VMEM((4, per_dev, 2 * extent, LANES), F32),
        ],
        compiler_params=pltpu.CompilerParams(vmem_limit_bytes=VMEM_LIMIT),
        name="poisson",
    )(mine[:, 0], mine[:, 1], jnp.asarray(eigen), jnp.asarray(left), jnp.asarray(sx2), jnp.asarray(sx3), jnp.asarray(lzx), incoming)
    back = lax.all_to_all(potential.reshape(owners, depth, rows, LANES), ("gz", "gy"), split_axis=0, concat_axis=0, tiled=True)

    term, part = pl.pallas_call(
        functools.partial(term_kernel, per_dev),
        grid=(depth,),
        out_shape=(
            jax.ShapeDtypeStruct((depth, rows, pairs, across), BF),
            jax.ShapeDtypeStruct((pairs, norb), F32),
        ),
        in_specs=[smem, smem, plane_spec, orb_spec, slab_spec],
        out_specs=(plane_spec, full((pairs, norb))),
        scratch_shapes=[pltpu.VMEM((rows * (pairs + GAP), LANES), F32)],
        compiler_params=params,
        name="term",
    )(ax, pair_live, psi, orbitals, back)
    shares = lax.all_to_all(part.reshape(owners, per_dev, norb), ("gz", "gy"), split_axis=0, concat_axis=0, tiled=True)
    summed = lax.all_gather(jnp.sum(shares, axis=0), ("gz", "gy"), axis=0, tiled=True)
    inner = lax.dot_general(
        summed, sel.astype(F32), (((0,), (0,)), ((), ())), precision=lax.Precision.HIGHEST, preferred_element_type=F32
    )
    tiles = (inner / (float(B) ** 3 / 4.0)).astype(BF)

    return pl.pallas_call(
        gradient_kernel,
        grid=(depth,),
        out_shape=jax.ShapeDtypeStruct(orbitals.shape, F32),
        in_specs=[
            full((pairs, norb)),
            full((norb, norb)),
            orb_spec,
            plane_spec,
        ],
        out_specs=orb_spec,
        compiler_params=params,
        name="gradient",
    )(hot_first, tiles, orbitals, term)


def solution(mesh):
    return jax.shard_map(
        body,
        mesh=mesh,
        in_specs=(P("gz", "gy", None, None), P(), P(), P()),
        out_specs=P("gz", "gy", None, None),
        check_vma=False,
    )
```

```python
import functools

import jax
import jax.numpy as jnp
import numpy as np
from jax import lax
from jax.experimental import pallas as pl
from jax.experimental.pallas import tpu as pltpu
from jax.sharding import PartitionSpec as P

B = 64
LANES = 128
GAP = 8
BF = jnp.bfloat16
F32 = jnp.float32
VMEM_LIMIT = 56 * 1024 * 1024


def dot_nt(a, b):
    return lax.dot_general(a, b, (((1,), (1,)), ((), ())), preferred_element_type=F32)


def dot_nn(a, b):
    return lax.dot_general(a, b, (((1,), (0,)), ((), ())), preferred_element_type=F32)


def dot_tn(a, b):
    return lax.dot_general(a, b, (((0,), (0,)), ((), ())), preferred_element_type=F32)


def split(a):
    hi = a.astype(BF)
    return hi, (a - hi.astype(F32)).astype(BF)


def density_kernel(per_dev, ax_ref, onehot_ref, orb_ref, out_ref, psi_ref, scr):
    _, rows, across, _ = orb_ref.shape
    pairs = onehot_ref.shape[0] // 2
    pitch = pairs + GAP
    owners = pairs // per_dev

    def row(y, _):
        both = dot_nt(onehot_ref[...], orb_ref[0, y])
        scr[pl.ds(pl.multiple_of(y * pitch, 8), pairs), :across] = both[:pairs] * both[pairs:]
        psi_ref[0, y] = both[pairs:].astype(BF)
        return 0

    lax.fori_loop(0, rows, row, 0, unroll=4)
    lane = lax.broadcasted_iota(jnp.int32, (rows, LANES), 1)

    def owner(d, _):
        acc = jnp.zeros((rows, LANES), F32)
        for s in range(per_dev):
            p = d * per_dev + s
            a = ax_ref[p]
            base = s * B
            x = scr[pl.ds(p, rows, stride=pitch), :]
            near = pltpu.roll(x, lax.rem(base - a + 2 * LANES, LANES), 1)
            far = pltpu.roll(x, lax.rem(base + across - a + 2 * LANES, LANES), 1)
            rel = lane - base
            acc = jnp.where((rel >= 0) & (rel < B), jnp.where(rel < across - a, near, far), acc)
        out_ref[d, 0] = acc.astype(BF)
        return 0

    lax.fori_loop(0, owners, owner, 0, unroll=4)


def poisson_kernel(per_dev, extent, chunks, az_ref, ay_ref, ly_ref, left_ref, sx2_ref, sx3_ref, lzx_ref, *refs):
    parts = refs[:len(chunks)]
    outs = refs[len(chunks):2 * len(chunks)]
    in_ref, field, ring, sems = refs[2 * len(chunks):]
    n_gz, n_gy, depth, rows, _ = in_ref.shape
    copies = [
        pltpu.make_async_copy(part, in_ref.at[:, :, start:start + size], sems.at[k])
        for k, (part, (start, size)) in enumerate(zip(parts, chunks))
    ]
    for copy in copies:
        copy.start()
    for copy in copies:
        copy.wait()
    lane = lax.broadcasted_iota(jnp.int32, (B, LANES), 1)
    lane_all = lax.broadcasted_iota(jnp.int32, (extent, LANES), 1)
    slots = ring.shape[0]
    pitch = B + GAP

    def along_rows(e):
        hi, lo = split(e)
        return dot_nn(left_ref[...], jnp.concatenate([hi, hi, lo], axis=0))

    def cut(a, slot):
        out = None
        for s in range(per_dev):
            z = lax.rem(az_ref[s] + a, extent)
            gz = z // depth
            zi = z - gz * depth
            for gy in range(n_gy):
                part = in_ref[gz, gy, zi].astype(F32)
                ring[slot, s, gy * rows:(gy + 1) * rows] = part
                ring[slot, s, extent + gy * rows:extent + (gy + 1) * rows] = part
            got = ring[slot, s, pl.ds(ay_ref[s], B), :]
            out = got if out is None else jnp.where(lane >= s * B, got, out)
        return out

    def first(step, _):
        for slot in range(slots):
            a = step * slots + slot
            d = cut(a, slot).astype(BF)
            e = dot_nn(jnp.concatenate([d, d], axis=1), sx2_ref[...])
            field[pl.ds(pl.multiple_of(a * pitch, 8), B), :] = along_rows(e)
        return 0

    lax.fori_loop(0, B // slots, first, 0)

    def middle(step, _):
        for k in range(4):
            y = step * 4 + k
            e = along_rows(field[pl.ds(y, B, stride=pitch), :])
            e = e / (lzx_ref[...] + ly_ref[y])
            field[pl.ds(y, B, stride=pitch), :] = along_rows(e)
        return 0

    lax.fori_loop(0, B // 4, middle, 0)

    def last(step, _):
        for k in range(4):
            a = step * 4 + k
            at = pl.ds(pl.multiple_of(a * pitch, 8), B)
            hi, lo = split(along_rows(field[at, :]))
            field[at, :] = dot_nn(jnp.concatenate([hi, hi, lo], axis=1), sx3_ref[...])
        return 0

    lax.fori_loop(0, B // 4, last, 0)
    ring[...] = jnp.zeros_like(ring)

    for out_ref, (start, size) in zip(outs, chunks):
        group = slots if (n_gz * size) % slots == 0 else 1

        def place(step, _):
            for slot in range(group):
                t = step * group + slot
                gz = t // size
                zi = t - gz * size
                z = gz * depth + start + zi
                out = jnp.zeros((extent, LANES), F32)
                for s in range(per_dev):
                    a = lax.rem(z - az_ref[s] + extent, extent)
                    v = field[pl.ds(pl.multiple_of(jnp.minimum(a, B - 1) * pitch, 8), B), :]
                    v = jnp.where(a < B, v, 0.0)
                    ring[slot, s, :B] = v
                    ring[slot, s, extent:extent + B] = v
                    got = ring[slot, s, pl.ds(extent - ay_ref[s], extent), :]
                    out = jnp.where(lane_all >= s * B, got, out)
                for gy in range(n_gy):
                    out_ref[gz, gy, zi] = out[gy * rows:(gy + 1) * rows].astype(BF)
            return 0

        lax.fori_loop(0, n_gz * size // group, place, 0)


def term_kernel(per_dev, ax_ref, live_ref, psi_ref, orb_ref, in_ref, *refs):
    _, rows, across, _ = orb_ref.shape
    term_ref, tile_ref, scr = refs[-3:]
    pairs = psi_ref.shape[2]
    pitch = pairs + GAP
    owners = pairs // per_dev
    lane = lax.broadcasted_iota(jnp.int32, (rows, LANES), 1)

    def owner(d, _):
        v = in_ref[d, 0].astype(F32)
        for s in range(per_dev):
            p = d * per_dev + s
            a = ax_ref[p]
            base = s * B
            near = pltpu.roll(v, lax.rem(a - base + 2 * LANES, LANES), 1)
            far = pltpu.roll(v, lax.rem(a - across - base + 3 * LANES, LANES), 1)
            rel = lane - a
            lit = live_ref[p] > 0
            v_p = jnp.where((rel >= 0) & (rel < B) & lit, near, 0.0)
            v_p = jnp.where((rel + across < B) & lit, far, v_p)
            scr[pl.ds(p, rows, stride=pitch), :] = v_p
        return 0

    lax.fori_loop(0, owners, owner, 0, unroll=4)

    @pl.when(pl.program_id(0) == 0)
    def _():
        tile_ref[...] = jnp.zeros_like(tile_ref)

    step = 4 if rows % 4 == 0 else 1

    def row(i, acc):
        for k in range(step):
            y = i * step + k
            v = scr[pl.ds(pl.multiple_of(y * pitch, 8), pairs), :across]
            t = (v * psi_ref[0, y].astype(F32)).astype(BF)
            term_ref[0, y] = t
            acc = acc + dot_nn(t, orb_ref[0, y])
        return acc

    tile_ref[...] += lax.fori_loop(0, rows // step, row, jnp.zeros(tile_ref.shape, F32))


def gradient_kernel(sel_ref, tiles_ref, orb_ref, term_ref, out_ref):
    _, rows, across, norb = orb_ref.shape
    step = 4 if rows % 4 == 0 else 1

    def some(i, _):
        at = pl.ds(i * step, step)
        o = orb_ref[0, at].reshape(step * across, norb)
        c = jnp.concatenate([term_ref[0, i * step + k].T for k in range(step)], axis=0)
        total = dot_nn(c, sel_ref[...]) - dot_nn(o, tiles_ref[...])
        out_ref[0, at] = total.reshape(step, across, norb)
        return 0

    lax.fori_loop(0, rows // step, some, 0, unroll=2)


def tables(per_dev):
    index = np.arange(1, B + 1, dtype=np.float64)
    s = np.sqrt(2.0 / (B + 1.0)) * np.sin(np.pi * index[:, None] * index[None, :] / (B + 1.0))
    eigen = 2.0 - 2.0 * np.cos(np.pi * index / (B + 1.0))
    hi = s.astype(jnp.bfloat16)
    lo = (s - hi.astype(np.float64)).astype(jnp.bfloat16)
    eye = np.eye(per_dev)
    bd = lambda m: np.kron(eye, m.astype(np.float32)).astype(jnp.bfloat16)
    left = np.concatenate([hi, lo, hi], axis=1)
    sx2 = np.concatenate([bd(hi), bd(lo)], axis=0)
    sx3 = np.concatenate([bd(hi), bd(lo), bd(hi)], axis=0)
    lzx = (eigen[:, None] + np.tile(eigen, per_dev)[None, :]).astype(np.float32)
    return eigen.astype(np.float32), left, sx2, sx3, lzx


def body(orbitals, pair_list, box_anchor, pair_live):
    depth, rows, across, norb = orbitals.shape
    n_gz = lax.axis_size("gz")
    n_gy = lax.axis_size("gy")
    owners = n_gz * n_gy
    pairs = pair_list.shape[0]
    per_dev = pairs // owners
    extent = depth * n_gz
    firsts = pair_list[:, 0]
    seconds = pair_list[:, 1]
    anchors = box_anchor[firsts]
    ax = anchors[:, 2]
    me = lax.axis_index(("gz", "gy"))
    mine = lax.dynamic_slice_in_dim(anchors, me * per_dev, per_dev, 0)
    orbs = jnp.arange(norb)
    sel = firsts[:, None] == orbs[None, :]
    hot_first = sel.astype(BF)
    hot_second = (seconds[:, None] == orbs[None, :]).astype(BF)
    hot_both = jnp.concatenate([hot_first, hot_second], axis=0)

    half = max(depth // 2, 1)
    chunks = [(start, size) for start, size in ((0, half), (half, depth - half)) if size]
    smem = pl.BlockSpec(memory_space=pltpu.SMEM)
    vmem = pl.BlockSpec(memory_space=pltpu.VMEM)
    hbm = pl.BlockSpec(memory_space=pl.ANY)
    full = lambda shape: pl.BlockSpec(shape, lambda z: (0,) * len(shape))
    planes = lambda start, *dims: pl.BlockSpec((1,) + dims, lambda z: (z + start,) + (0,) * len(dims))
    slab_spec = pl.BlockSpec((owners, 1, rows, LANES), lambda z: (0, z, 0, 0))
    params = pltpu.CompilerParams(dimension_semantics=("arbitrary",), vmem_limit_bytes=VMEM_LIMIT)
    cells = rows * across

    incoming, psis = [], []
    for start, size in chunks:
        density, psi = pl.pallas_call(
            functools.partial(density_kernel, per_dev),
            grid=(size,),
            out_shape=(
                jax.ShapeDtypeStruct((owners, size, rows, LANES), BF),
                jax.ShapeDtypeStruct((size, rows, pairs, across), BF),
            ),
            in_specs=[smem, full((2 * pairs, norb)), planes(start, rows, across, norb)],
            out_specs=(slab_spec, planes(0, rows, pairs, across)),
            scratch_shapes=[pltpu.VMEM((rows * (pairs + GAP), LANES), F32)],
            compiler_params=params,
            cost_estimate=pl.CostEstimate(
                flops=4 * size * cells * norb * pairs, bytes_accessed=16 * size * cells * norb, transcendentals=0
            ),
            name="density",
        )(ax, hot_both, orbitals)
        got = lax.all_to_all(density, ("gz", "gy"), split_axis=0, concat_axis=0, tiled=True)
        incoming.append(got.reshape(n_gz, n_gy, size, rows, LANES))
        psis.append(psi)

    eigen, left, sx2, sx3, lzx = tables(per_dev)
    potential = pl.pallas_call(
        functools.partial(poisson_kernel, per_dev, extent, chunks),
        out_shape=[jax.ShapeDtypeStruct(got.shape, BF) for got in incoming],
        in_specs=[smem, smem, smem, vmem, vmem, vmem, vmem] + [hbm] * len(chunks),
        out_specs=[vmem] * len(chunks),
        scratch_shapes=[
            pltpu.VMEM((n_gz, n_gy, depth, rows, LANES), BF),
            pltpu.VMEM((B * (B + GAP), LANES), F32),
            pltpu.VMEM((4, per_dev, 2 * extent, LANES), F32),
            pltpu.SemaphoreType.DMA((len(chunks),)),
        ],
        compiler_params=pltpu.CompilerParams(vmem_limit_bytes=VMEM_LIMIT),
        name="poisson",
    )(mine[:, 0], mine[:, 1], jnp.asarray(eigen), jnp.asarray(left), jnp.asarray(sx2), jnp.asarray(sx3), jnp.asarray(lzx), *incoming)

    term, part = None, 0.0
    for (start, size), psi, field in zip(chunks, psis, potential):
        back = lax.all_to_all(
            field.reshape(owners, size, rows, LANES), ("gz", "gy"), split_axis=0, concat_axis=0, tiled=True
        )
        held = [] if term is None else [term]
        term, share = pl.pallas_call(
            functools.partial(term_kernel, per_dev),
            grid=(size,),
            out_shape=(
                jax.ShapeDtypeStruct((depth, rows, pairs, across), BF),
                jax.ShapeDtypeStruct((pairs, norb), F32),
            ),
            in_specs=[
                smem,
                smem,
                planes(0, rows, pairs, across),
                planes(start, rows, across, norb),
                slab_spec,
            ] + [hbm] * len(held),
            out_specs=(planes(start, rows, pairs, across), full((pairs, norb))),
            scratch_shapes=[pltpu.VMEM((rows * (pairs + GAP), LANES), F32)],
            input_output_aliases={5: 0} if held else {},
            compiler_params=params,
            cost_estimate=pl.CostEstimate(
                flops=2 * size * cells * norb * pairs, bytes_accessed=16 * size * cells * norb, transcendentals=0
            ),
            name="term",
        )(ax, pair_live, psi, orbitals, back, *held)
        part = part + share
    whole = lambda x: lax.all_to_all(x, ("gz", "gy"), split_axis=0, concat_axis=0, tiled=True)
    shares = whole(part.reshape(owners, per_dev, norb))
    mine_sum = jnp.sum(shares, axis=0, keepdims=True)
    summed = whole(jnp.broadcast_to(mine_sum, shares.shape)).reshape(pairs, norb)
    inner = lax.dot_general(
        summed, sel.astype(F32), (((0,), (0,)), ((), ())), precision=lax.Precision.HIGHEST, preferred_element_type=F32
    )
    tiles = (inner / (float(B) ** 3 / 4.0)).astype(BF)

    return pl.pallas_call(
        gradient_kernel,
        grid=(depth,),
        out_shape=jax.ShapeDtypeStruct(orbitals.shape, F32),
        in_specs=[
            full((pairs, norb)),
            full((norb, norb)),
            planes(0, rows, across, norb),
            planes(0, rows, pairs, across),
        ],
        out_specs=planes(0, rows, across, norb),
        compiler_params=params,
        name="gradient",
    )(hot_first, tiles, orbitals, term)


def solution(mesh):
    return jax.shard_map(
        body,
        mesh=mesh,
        in_specs=(P("gz", "gy", None, None), P(), P(), P()),
        out_specs=P("gz", "gy", None, None),
        check_vma=False,
    )
```

```python
import functools

import jax
import jax.numpy as jnp
import numpy as np
from jax import lax
from jax.experimental import pallas as pl
from jax.experimental.pallas import tpu as pltpu
from jax.sharding import PartitionSpec as P

B = 64
LANES = 128
GAP = 8
BF = jnp.bfloat16
F32 = jnp.float32
VMEM_LIMIT = 56 * 1024 * 1024


def dot_nt(a, b):
    return lax.dot_general(a, b, (((1,), (1,)), ((), ())), preferred_element_type=F32)


def dot_nn(a, b):
    return lax.dot_general(a, b, (((1,), (0,)), ((), ())), preferred_element_type=F32)


def dot_tn(a, b):
    return lax.dot_general(a, b, (((0,), (0,)), ((), ())), preferred_element_type=F32)


def split(a):
    hi = a.astype(BF)
    return hi, (a - hi.astype(F32)).astype(BF)


def density_kernel(per_dev, ax_ref, onehot_ref, orb_ref, out_ref, psi_ref, scr):
    _, rows, across, _ = orb_ref.shape
    pairs = onehot_ref.shape[0] // 2
    pitch = pairs + GAP
    owners = pairs // per_dev

    def row(y, carry):
        both = dot_nt(onehot_ref[...], orb_ref[0, y])
        value = both[:pairs] * both[pairs:] + carry
        sent = value.astype(BF).astype(F32)
        scr[pl.ds(pl.multiple_of(y * pitch, 8), pairs), :across] = sent
        psi_ref[0, y] = both[pairs:].astype(BF)
        return value - sent

    lax.fori_loop(0, rows, row, jnp.zeros((pairs, across), F32), unroll=4)
    lane = lax.broadcasted_iota(jnp.int32, (rows, LANES), 1)

    def owner(d, _):
        acc = jnp.zeros((rows, LANES), F32)
        for s in range(per_dev):
            p = d * per_dev + s
            a = ax_ref[p]
            base = s * B
            x = scr[pl.ds(p, rows, stride=pitch), :]
            near = pltpu.roll(x, lax.rem(base - a + 2 * LANES, LANES), 1)
            far = pltpu.roll(x, lax.rem(base + across - a + 2 * LANES, LANES), 1)
            rel = lane - base
            acc = jnp.where((rel >= 0) & (rel < B), jnp.where(rel < across - a, near, far), acc)
        out_ref[d, 0] = acc.astype(BF)
        return 0

    lax.fori_loop(0, owners, owner, 0, unroll=4)


def poisson_kernel(per_dev, extent, chunks, az_ref, ay_ref, ly_ref, left_ref, sx2_ref, sx3_ref, lzx_ref, *refs):
    parts = refs[:len(chunks)]
    outs = refs[len(chunks):2 * len(chunks)]
    in_ref, field, ring, sems = refs[2 * len(chunks):]
    n_gz, n_gy, depth, rows, _ = in_ref.shape
    copies = [
        pltpu.make_async_copy(part, in_ref.at[:, :, start:start + size], sems.at[k])
        for k, (part, (start, size)) in enumerate(zip(parts, chunks))
    ]
    for copy in copies:
        copy.start()
    for copy in copies:
        copy.wait()
    lane = lax.broadcasted_iota(jnp.int32, (B, LANES), 1)
    lane_all = lax.broadcasted_iota(jnp.int32, (extent, LANES), 1)
    slots = ring.shape[0]
    pitch = B + GAP

    def along_rows(e):
        hi, lo = split(e)
        return dot_nn(left_ref[...], jnp.concatenate([hi, hi, lo], axis=0))

    def cut(a, slot):
        out = None
        for s in range(per_dev):
            z = lax.rem(az_ref[s] + a, extent)
            gz = z // depth
            zi = z - gz * depth
            for gy in range(n_gy):
                part = in_ref[gz, gy, zi].astype(F32)
                ring[slot, s, gy * rows:(gy + 1) * rows] = part
                ring[slot, s, extent + gy * rows:extent + (gy + 1) * rows] = part
            got = ring[slot, s, pl.ds(ay_ref[s], B), :]
            out = got if out is None else jnp.where(lane >= s * B, got, out)
        return out

    def first(step, _):
        for slot in range(slots):
            a = step * slots + slot
            d = cut(a, slot).astype(BF)
            e = dot_nn(jnp.concatenate([d, d], axis=1), sx2_ref[...])
            field[pl.ds(pl.multiple_of(a * pitch, 8), B), :] = along_rows(e)
        return 0

    lax.fori_loop(0, B // slots, first, 0)

    def middle(step, _):
        for k in range(4):
            y = step * 4 + k
            e = along_rows(field[pl.ds(y, B, stride=pitch), :])
            e = e / (lzx_ref[...] + ly_ref[y])
            field[pl.ds(y, B, stride=pitch), :] = along_rows(e)
        return 0

    lax.fori_loop(0, B // 4, middle, 0)

    def last(step, _):
        for k in range(4):
            a = step * 4 + k
            at = pl.ds(pl.multiple_of(a * pitch, 8), B)
            hi, lo = split(along_rows(field[at, :]))
            field[at, :] = dot_nn(jnp.concatenate([hi, hi, lo], axis=1), sx3_ref[...])
        return 0

    lax.fori_loop(0, B // 4, last, 0)
    ring[...] = jnp.zeros_like(ring)

    for out_ref, (start, size) in zip(outs, chunks):
        group = slots if (n_gz * size) % slots == 0 else 1

        def place(step, carry):
            for slot in range(group):
                t = step * group + slot
                gz = t // size
                zi = t - gz * size
                z = gz * depth + start + zi
                out = jnp.zeros((extent, LANES), F32)
                inside = jnp.zeros((extent, LANES), F32)
                for s in range(per_dev):
                    a = lax.rem(z - az_ref[s] + extent, extent)
                    v = field[pl.ds(pl.multiple_of(jnp.minimum(a, B - 1) * pitch, 8), B), :]
                    v = jnp.where(a < B, v, 0.0)
                    ring[slot, s, :B] = v
                    ring[slot, s, extent:extent + B] = v
                    got = ring[slot, s, pl.ds(extent - ay_ref[s], extent), :]
                    out = jnp.where(lane_all >= s * B, got, out)
                    inside = jnp.where(lane_all >= s * B, (a < B).astype(F32), inside)
                out = out + carry * inside
                sent = out.astype(BF)
                carry = (out - sent.astype(F32)) * inside
                for gy in range(n_gy):
                    out_ref[gz, gy, zi] = sent[gy * rows:(gy + 1) * rows]
            return carry

        lax.fori_loop(0, n_gz * size // group, place, jnp.zeros((extent, LANES), F32))


def term_kernel(per_dev, ax_ref, live_ref, psi_ref, orb_ref, in_ref, *refs):
    _, rows, across, _ = orb_ref.shape
    term_ref, tile_ref, scr = refs[-3:]
    pairs = psi_ref.shape[2]
    pitch = pairs + GAP
    owners = pairs // per_dev
    lane = lax.broadcasted_iota(jnp.int32, (rows, LANES), 1)

    def owner(d, _):
        v = in_ref[d, 0].astype(F32)
        for s in range(per_dev):
            p = d * per_dev + s
            a = ax_ref[p]
            base = s * B
            near = pltpu.roll(v, lax.rem(a - base + 2 * LANES, LANES), 1)
            far = pltpu.roll(v, lax.rem(a - across - base + 3 * LANES, LANES), 1)
            rel = lane - a
            lit = live_ref[p] > 0
            v_p = jnp.where((rel >= 0) & (rel < B) & lit, near, 0.0)
            v_p = jnp.where((rel + across < B) & lit, far, v_p)
            scr[pl.ds(p, rows, stride=pitch), :] = v_p
        return 0

    lax.fori_loop(0, owners, owner, 0, unroll=4)

    @pl.when(pl.program_id(0) == 0)
    def _():
        tile_ref[...] = jnp.zeros_like(tile_ref)

    step = 4 if rows % 4 == 0 else 1

    def row(i, acc):
        for k in range(step):
            y = i * step + k
            v = scr[pl.ds(pl.multiple_of(y * pitch, 8), pairs), :across]
            t = (v * psi_ref[0, y].astype(F32)).astype(BF)
            term_ref[0, y] = t
            acc = acc + dot_nn(t, orb_ref[0, y])
        return acc

    tile_ref[...] += lax.fori_loop(0, rows // step, row, jnp.zeros(tile_ref.shape, F32))


def gradient_kernel(sel_ref, tiles_ref, orb_ref, term_ref, out_ref):
    _, rows, across, norb = orb_ref.shape
    step = 4 if rows % 4 == 0 else 1

    def some(i, _):
        at = pl.ds(i * step, step)
        o = orb_ref[0, at].reshape(step * across, norb)
        c = jnp.concatenate([term_ref[0, i * step + k].T for k in range(step)], axis=0)
        total = dot_nn(c, sel_ref[...]) - dot_nn(o, tiles_ref[...])
        out_ref[0, at] = total.reshape(step, across, norb)
        return 0

    lax.fori_loop(0, rows // step, some, 0, unroll=2)


def tables(per_dev):
    index = np.arange(1, B + 1, dtype=np.float64)
    s = np.sqrt(2.0 / (B + 1.0)) * np.sin(np.pi * index[:, None] * index[None, :] / (B + 1.0))
    eigen = 2.0 - 2.0 * np.cos(np.pi * index / (B + 1.0))
    hi = s.astype(jnp.bfloat16)
    lo = (s - hi.astype(np.float64)).astype(jnp.bfloat16)
    eye = np.eye(per_dev)
    bd = lambda m: np.kron(eye, m.astype(np.float32)).astype(jnp.bfloat16)
    left = np.concatenate([hi, lo, hi], axis=1)
    sx2 = np.concatenate([bd(hi), bd(lo)], axis=0)
    sx3 = np.concatenate([bd(hi), bd(lo), bd(hi)], axis=0)
    lzx = (eigen[:, None] + np.tile(eigen, per_dev)[None, :]).astype(np.float32)
    return eigen.astype(np.float32), left, sx2, sx3, lzx


def body(orbitals, pair_list, box_anchor, pair_live):
    depth, rows, across, norb = orbitals.shape
    n_gz = lax.axis_size("gz")
    n_gy = lax.axis_size("gy")
    owners = n_gz * n_gy
    pairs = pair_list.shape[0]
    per_dev = pairs // owners
    extent = depth * n_gz
    firsts = pair_list[:, 0]
    seconds = pair_list[:, 1]
    anchors = box_anchor[firsts]
    ax = anchors[:, 2]
    me = lax.axis_index(("gz", "gy"))
    mine = lax.dynamic_slice_in_dim(anchors, me * per_dev, per_dev, 0)
    orbs = jnp.arange(norb)
    sel = firsts[:, None] == orbs[None, :]
    hot_first = sel.astype(BF)
    hot_second = (seconds[:, None] == orbs[None, :]).astype(BF)
    hot_both = jnp.concatenate([hot_first, hot_second], axis=0)

    lead = max(depth // 3, 1)
    chunks = [(start, size) for start, size in ((0, lead), (lead, depth - lead)) if size]
    smem = pl.BlockSpec(memory_space=pltpu.SMEM)
    vmem = pl.BlockSpec(memory_space=pltpu.VMEM)
    hbm = pl.BlockSpec(memory_space=pl.ANY)
    full = lambda shape: pl.BlockSpec(shape, lambda z: (0,) * len(shape))
    planes = lambda start, *dims: pl.BlockSpec((1,) + dims, lambda z: (z + start,) + (0,) * len(dims))
    slab_spec = pl.BlockSpec((owners, 1, rows, LANES), lambda z: (0, z, 0, 0))
    params = pltpu.CompilerParams(dimension_semantics=("arbitrary",), vmem_limit_bytes=VMEM_LIMIT)
    cells = rows * across

    incoming, psis = [], []
    for start, size in chunks:
        density, psi = pl.pallas_call(
            functools.partial(density_kernel, per_dev),
            grid=(size,),
            out_shape=(
                jax.ShapeDtypeStruct((owners, size, rows, LANES), BF),
                jax.ShapeDtypeStruct((size, rows, pairs, across), BF),
            ),
            in_specs=[smem, full((2 * pairs, norb)), planes(start, rows, across, norb)],
            out_specs=(slab_spec, planes(0, rows, pairs, across)),
            scratch_shapes=[pltpu.VMEM((rows * (pairs + GAP), LANES), F32)],
            compiler_params=params,
            cost_estimate=pl.CostEstimate(
                flops=4 * size * cells * norb * pairs, bytes_accessed=16 * size * cells * norb, transcendentals=0
            ),
            name="density",
        )(ax, hot_both, orbitals)
        got = lax.all_to_all(density, ("gz", "gy"), split_axis=0, concat_axis=0, tiled=True)
        incoming.append(got.reshape(n_gz, n_gy, size, rows, LANES))
        psis.append(psi)

    eigen, left, sx2, sx3, lzx = tables(per_dev)
    potential = pl.pallas_call(
        functools.partial(poisson_kernel, per_dev, extent, chunks),
        out_shape=[jax.ShapeDtypeStruct(got.shape, BF) for got in incoming],
        in_specs=[smem, smem, smem, vmem, vmem, vmem, vmem] + [hbm] * len(chunks),
        out_specs=[vmem] * len(chunks),
        scratch_shapes=[
            pltpu.VMEM((n_gz, n_gy, depth, rows, LANES), BF),
            pltpu.VMEM((B * (B + GAP), LANES), F32),
            pltpu.VMEM((4, per_dev, 2 * extent, LANES), F32),
            pltpu.SemaphoreType.DMA((len(chunks),)),
        ],
        compiler_params=pltpu.CompilerParams(vmem_limit_bytes=VMEM_LIMIT),
        name="poisson",
    )(mine[:, 0], mine[:, 1], jnp.asarray(eigen), jnp.asarray(left), jnp.asarray(sx2), jnp.asarray(sx3), jnp.asarray(lzx), *incoming)

    term, part = None, 0.0
    for (start, size), psi, field in reversed(list(zip(chunks, psis, potential))):
        back = lax.all_to_all(
            field.reshape(owners, size, rows, LANES), ("gz", "gy"), split_axis=0, concat_axis=0, tiled=True
        )
        held = [] if term is None else [term]
        term, share = pl.pallas_call(
            functools.partial(term_kernel, per_dev),
            grid=(size,),
            out_shape=(
                jax.ShapeDtypeStruct((depth, rows, pairs, across), BF),
                jax.ShapeDtypeStruct((pairs, norb), F32),
            ),
            in_specs=[
                smem,
                smem,
                planes(0, rows, pairs, across),
                planes(start, rows, across, norb),
                slab_spec,
            ] + [hbm] * len(held),
            out_specs=(planes(start, rows, pairs, across), full((pairs, norb))),
            scratch_shapes=[pltpu.VMEM((rows * (pairs + GAP), LANES), F32)],
            input_output_aliases={5: 0} if held else {},
            compiler_params=params,
            cost_estimate=pl.CostEstimate(
                flops=2 * size * cells * norb * pairs, bytes_accessed=16 * size * cells * norb, transcendentals=0
            ),
            name="term",
        )(ax, pair_live, psi, orbitals, back, *held)
        part = part + share
    whole = lambda x: lax.all_to_all(x, ("gz", "gy"), split_axis=0, concat_axis=0, tiled=True)
    shares = whole(part.reshape(owners, per_dev, norb))
    mine_sum = jnp.sum(shares, axis=0, keepdims=True)
    summed = whole(jnp.broadcast_to(mine_sum, shares.shape)).reshape(pairs, norb)
    inner = lax.dot_general(
        summed, sel.astype(F32), (((0,), (0,)), ((), ())), precision=lax.Precision.HIGHEST, preferred_element_type=F32
    )
    tiles = (inner / (float(B) ** 3 / 4.0)).astype(BF)

    return pl.pallas_call(
        gradient_kernel,
        grid=(depth,),
        out_shape=jax.ShapeDtypeStruct(orbitals.shape, F32),
        in_specs=[
            full((pairs, norb)),
            full((norb, norb)),
            planes(0, rows, across, norb),
            planes(0, rows, pairs, across),
        ],
        out_specs=planes(0, rows, across, norb),
        compiler_params=params,
        name="gradient",
    )(hot_first, tiles, orbitals, term)


def solution(mesh):
    return jax.shard_map(
        body,
        mesh=mesh,
        in_specs=(P("gz", "gy", None, None), P(), P(), P()),
        out_specs=P("gz", "gy", None, None),
        check_vma=False,
    )
```

```python
import functools

import jax
import jax.numpy as jnp
import numpy as np
from jax import lax
from jax.experimental import pallas as pl
from jax.experimental.pallas import tpu as pltpu
from jax.sharding import PartitionSpec as P

B = 64
LANES = 128
GAP = 8
BF = jnp.bfloat16
F32 = jnp.float32
VMEM_LIMIT = 56 * 1024 * 1024


def dot_nt(a, b):
    return lax.dot_general(a, b, (((1,), (1,)), ((), ())), preferred_element_type=F32)


def dot_nn(a, b):
    return lax.dot_general(a, b, (((1,), (0,)), ((), ())), preferred_element_type=F32)


def dot_tn(a, b):
    return lax.dot_general(a, b, (((0,), (0,)), ((), ())), preferred_element_type=F32)


def split(a):
    hi = a.astype(BF)
    return hi, (a - hi.astype(F32)).astype(BF)


def density_kernel(per_dev, ax_ref, onehot_ref, orb_ref, out_ref, psi_ref, scr):
    _, rows, across, _ = orb_ref.shape
    pairs = onehot_ref.shape[0] // 2
    pitch = pairs + GAP
    owners = pairs // per_dev

    def row(y, carry):
        both = dot_nt(onehot_ref[...], orb_ref[0, y])
        value = both[:pairs] * both[pairs:] + carry
        sent = value.astype(BF).astype(F32)
        scr[pl.ds(pl.multiple_of(y * pitch, 8), pairs), :across] = sent
        psi_ref[0, y] = both[pairs:].astype(BF)
        return value - sent

    lax.fori_loop(0, rows, row, jnp.zeros((pairs, across), F32), unroll=4)
    lane = lax.broadcasted_iota(jnp.int32, (rows, LANES), 1)

    def owner(d, _):
        acc = jnp.zeros((rows, LANES), F32)
        for s in range(per_dev):
            p = d * per_dev + s
            a = ax_ref[p]
            base = s * B
            x = scr[pl.ds(p, rows, stride=pitch), :]
            near = pltpu.roll(x, lax.rem(base - a + 2 * LANES, LANES), 1)
            far = pltpu.roll(x, lax.rem(base + across - a + 2 * LANES, LANES), 1)
            rel = lane - base
            acc = jnp.where((rel >= 0) & (rel < B), jnp.where(rel < across - a, near, far), acc)
        out_ref[d, 0] = acc.astype(BF)
        return 0

    lax.fori_loop(0, owners, owner, 0, unroll=4)


def poisson_kernel(per_dev, extent, chunks, az_ref, ay_ref, ly_ref, left_ref, sx2_ref, sx3_ref, lzx_ref, *refs):
    parts = refs[:len(chunks)]
    outs = refs[len(chunks):2 * len(chunks)]
    in_ref, field, ring, sems = refs[2 * len(chunks):]
    n_gz, n_gy, depth, rows, _ = in_ref.shape
    copies = [
        pltpu.make_async_copy(part, in_ref.at[:, :, start:start + size], sems.at[k])
        for k, (part, (start, size)) in enumerate(zip(parts, chunks))
    ]
    for copy in copies:
        copy.start()
    for copy in copies:
        copy.wait()
    lane = lax.broadcasted_iota(jnp.int32, (B, LANES), 1)
    lane_all = lax.broadcasted_iota(jnp.int32, (extent, LANES), 1)
    slots = ring.shape[0]
    pitch = B + GAP

    def along_rows(blocks):
        hi, lo = split(jnp.concatenate(blocks, axis=1))
        wide = dot_nn(left_ref[...], jnp.concatenate([hi, hi, lo], axis=0))
        return [wide[:, k * LANES:(k + 1) * LANES] for k in range(len(blocks))]

    def cut(a, slot):
        out = None
        for s in range(per_dev):
            z = lax.rem(az_ref[s] + a, extent)
            gz = z // depth
            zi = z - gz * depth
            for gy in range(n_gy):
                part = in_ref[gz, gy, zi].astype(F32)
                ring[slot, s, gy * rows:(gy + 1) * rows] = part
                ring[slot, s, extent + gy * rows:extent + (gy + 1) * rows] = part
            got = ring[slot, s, pl.ds(ay_ref[s], B), :]
            out = got if out is None else jnp.where(lane >= s * B, got, out)
        return out

    def first(step, _):
        d = jnp.concatenate([cut(step * slots + slot, slot).astype(BF) for slot in range(slots)], axis=0)
        e = dot_nn(jnp.concatenate([d, d], axis=1), sx2_ref[...])
        moved = along_rows([e[slot * B:(slot + 1) * B] for slot in range(slots)])
        for slot in range(slots):
            field[pl.ds(pl.multiple_of((step * slots + slot) * pitch, 8), B), :] = moved[slot]
        return 0

    lax.fori_loop(0, B // slots, first, 0)

    def middle(step, _):
        at = [step * slots + k for k in range(slots)]
        modes = along_rows([field[pl.ds(y, B, stride=pitch), :] for y in at])
        solved = along_rows([e / (lzx_ref[...] + ly_ref[y]) for e, y in zip(modes, at)])
        for y, e in zip(at, solved):
            field[pl.ds(y, B, stride=pitch), :] = e
        return 0

    lax.fori_loop(0, B // slots, middle, 0, unroll=2)

    def last(step, _):
        at = [pl.ds(pl.multiple_of((step * slots + k) * pitch, 8), B) for k in range(slots)]
        hi, lo = split(jnp.concatenate(along_rows([field[a, :] for a in at]), axis=0))
        e = dot_nn(jnp.concatenate([hi, hi, lo], axis=1), sx3_ref[...])
        for k in range(slots):
            field[at[k], :] = e[k * B:(k + 1) * B]
        return 0

    lax.fori_loop(0, B // slots, last, 0, unroll=2)
    ring[...] = jnp.zeros_like(ring)

    for out_ref, (start, size) in zip(outs, chunks):
        group = slots if (n_gz * size) % slots == 0 else 1

        def place(step, carry):
            for slot in range(group):
                t = step * group + slot
                gz = t // size
                zi = t - gz * size
                z = gz * depth + start + zi
                out = jnp.zeros((extent, LANES), F32)
                inside = jnp.zeros((extent, LANES), F32)
                for s in range(per_dev):
                    a = lax.rem(z - az_ref[s] + extent, extent)
                    v = field[pl.ds(pl.multiple_of(jnp.minimum(a, B - 1) * pitch, 8), B), :]
                    v = jnp.where(a < B, v, 0.0)
                    ring[slot, s, :B] = v
                    ring[slot, s, extent:extent + B] = v
                    got = ring[slot, s, pl.ds(extent - ay_ref[s], extent), :]
                    out = jnp.where(lane_all >= s * B, got, out)
                    inside = jnp.where(lane_all >= s * B, (a < B).astype(F32), inside)
                out = out + carry * inside
                sent = out.astype(BF)
                carry = (out - sent.astype(F32)) * inside
                for gy in range(n_gy):
                    out_ref[gz, gy, zi] = sent[gy * rows:(gy + 1) * rows]
            return carry

        lax.fori_loop(0, n_gz * size // group, place, jnp.zeros((extent, LANES), F32))


def term_kernel(per_dev, ax_ref, live_ref, psi_ref, orb_ref, in_ref, *refs):
    _, rows, across, _ = orb_ref.shape
    term_ref, tile_ref, scr = refs[-3:]
    pairs = psi_ref.shape[2]
    pitch = pairs + GAP
    owners = pairs // per_dev
    lane = lax.broadcasted_iota(jnp.int32, (rows, LANES), 1)

    def owner(d, _):
        v = in_ref[d, 0].astype(F32)
        for s in range(per_dev):
            p = d * per_dev + s
            a = ax_ref[p]
            base = s * B
            near = pltpu.roll(v, lax.rem(a - base + 2 * LANES, LANES), 1)
            far = pltpu.roll(v, lax.rem(a - across - base + 3 * LANES, LANES), 1)
            rel = lane - a
            lit = live_ref[p] > 0
            v_p = jnp.where((rel >= 0) & (rel < B) & lit, near, 0.0)
            v_p = jnp.where((rel + across < B) & lit, far, v_p)
            scr[pl.ds(p, rows, stride=pitch), :] = v_p
        return 0

    lax.fori_loop(0, owners, owner, 0, unroll=4)

    @pl.when(pl.program_id(0) == 0)
    def _():
        tile_ref[...] = jnp.zeros_like(tile_ref)

    step = 4 if rows % 4 == 0 else 1

    def row(i, acc):
        for k in range(step):
            y = i * step + k
            v = scr[pl.ds(pl.multiple_of(y * pitch, 8), pairs), :across]
            t = (v * psi_ref[0, y].astype(F32)).astype(BF)
            term_ref[0, y] = t
            acc = acc + dot_nn(t, orb_ref[0, y])
        return acc

    tile_ref[...] += lax.fori_loop(0, rows // step, row, jnp.zeros(tile_ref.shape, F32))


def gradient_kernel(sel_ref, tiles_ref, orb_ref, term_ref, out_ref):
    _, rows, across, norb = orb_ref.shape
    step = 4 if rows % 4 == 0 else 1

    def some(i, _):
        at = pl.ds(i * step, step)
        o = orb_ref[0, at].reshape(step * across, norb)
        c = jnp.concatenate([term_ref[0, i * step + k].T for k in range(step)], axis=0)
        total = dot_nn(c, sel_ref[...]) - dot_nn(o, tiles_ref[...])
        out_ref[0, at] = total.reshape(step, across, norb)
        return 0

    lax.fori_loop(0, rows // step, some, 0, unroll=2)


def tables(per_dev):
    index = np.arange(1, B + 1, dtype=np.float64)
    s = np.sqrt(2.0 / (B + 1.0)) * np.sin(np.pi * index[:, None] * index[None, :] / (B + 1.0))
    eigen = 2.0 - 2.0 * np.cos(np.pi * index / (B + 1.0))
    hi = s.astype(jnp.bfloat16)
    lo = (s - hi.astype(np.float64)).astype(jnp.bfloat16)
    eye = np.eye(per_dev)
    bd = lambda m: np.kron(eye, m.astype(np.float32)).astype(jnp.bfloat16)
    left = np.concatenate([hi, lo, hi], axis=1)
    sx2 = np.concatenate([bd(hi), bd(lo)], axis=0)
    sx3 = np.concatenate([bd(hi), bd(lo), bd(hi)], axis=0)
    lzx = (eigen[:, None] + np.tile(eigen, per_dev)[None, :]).astype(np.float32)
    return eigen.astype(np.float32), left, sx2, sx3, lzx


def body(orbitals, pair_list, box_anchor, pair_live):
    depth, rows, across, norb = orbitals.shape
    n_gz = lax.axis_size("gz")
    n_gy = lax.axis_size("gy")
    owners = n_gz * n_gy
    pairs = pair_list.shape[0]
    per_dev = pairs // owners
    extent = depth * n_gz
    firsts = pair_list[:, 0]
    seconds = pair_list[:, 1]
    anchors = box_anchor[firsts]
    ax = anchors[:, 2]
    me = lax.axis_index(("gz", "gy"))
    mine = lax.dynamic_slice_in_dim(anchors, me * per_dev, per_dev, 0)
    orbs = jnp.arange(norb)
    sel = firsts[:, None] == orbs[None, :]
    hot_first = sel.astype(BF)
    hot_second = (seconds[:, None] == orbs[None, :]).astype(BF)
    hot_both = jnp.concatenate([hot_first, hot_second], axis=0)

    lead = max(depth // 3, 1)
    chunks = [(start, size) for start, size in ((0, lead), (lead, depth - lead)) if size]
    smem = pl.BlockSpec(memory_space=pltpu.SMEM)
    vmem = pl.BlockSpec(memory_space=pltpu.VMEM)
    hbm = pl.BlockSpec(memory_space=pl.ANY)
    full = lambda shape: pl.BlockSpec(shape, lambda z: (0,) * len(shape))
    planes = lambda start, *dims: pl.BlockSpec((1,) + dims, lambda z: (z + start,) + (0,) * len(dims))
    slab_spec = pl.BlockSpec((owners, 1, rows, LANES), lambda z: (0, z, 0, 0))
    params = pltpu.CompilerParams(dimension_semantics=("arbitrary",), vmem_limit_bytes=VMEM_LIMIT)
    cells = rows * across

    incoming, psis = [], []
    for start, size in chunks:
        density, psi = pl.pallas_call(
            functools.partial(density_kernel, per_dev),
            grid=(size,),
            out_shape=(
                jax.ShapeDtypeStruct((owners, size, rows, LANES), BF),
                jax.ShapeDtypeStruct((size, rows, pairs, across), BF),
            ),
            in_specs=[smem, full((2 * pairs, norb)), planes(start, rows, across, norb)],
            out_specs=(slab_spec, planes(0, rows, pairs, across)),
            scratch_shapes=[pltpu.VMEM((rows * (pairs + GAP), LANES), F32)],
            compiler_params=params,
            cost_estimate=pl.CostEstimate(
                flops=4 * size * cells * norb * pairs, bytes_accessed=16 * size * cells * norb, transcendentals=0
            ),
            name="density",
        )(ax, hot_both, orbitals)
        got = lax.all_to_all(density, ("gz", "gy"), split_axis=0, concat_axis=0, tiled=True)
        incoming.append(got.reshape(n_gz, n_gy, size, rows, LANES))
        psis.append(psi)

    eigen, left, sx2, sx3, lzx = tables(per_dev)
    potential = pl.pallas_call(
        functools.partial(poisson_kernel, per_dev, extent, chunks),
        out_shape=[jax.ShapeDtypeStruct(got.shape, BF) for got in incoming],
        in_specs=[smem, smem, smem, vmem, vmem, vmem, vmem] + [hbm] * len(chunks),
        out_specs=[vmem] * len(chunks),
        scratch_shapes=[
            pltpu.VMEM((n_gz, n_gy, depth, rows, LANES), BF),
            pltpu.VMEM((B * (B + GAP), LANES), F32),
            pltpu.VMEM((4, per_dev, 2 * extent, LANES), F32),
            pltpu.SemaphoreType.DMA((len(chunks),)),
        ],
        compiler_params=pltpu.CompilerParams(vmem_limit_bytes=VMEM_LIMIT),
        name="poisson",
    )(mine[:, 0], mine[:, 1], jnp.asarray(eigen), jnp.asarray(left), jnp.asarray(sx2), jnp.asarray(sx3), jnp.asarray(lzx), *incoming)

    term, part = None, 0.0
    for (start, size), psi, field in reversed(list(zip(chunks, psis, potential))):
        back = lax.all_to_all(
            field.reshape(owners, size, rows, LANES), ("gz", "gy"), split_axis=0, concat_axis=0, tiled=True
        )
        held = [] if term is None else [term]
        term, share = pl.pallas_call(
            functools.partial(term_kernel, per_dev),
            grid=(size,),
            out_shape=(
                jax.ShapeDtypeStruct((depth, rows, pairs, across), BF),
                jax.ShapeDtypeStruct((pairs, norb), F32),
            ),
            in_specs=[
                smem,
                smem,
                planes(0, rows, pairs, across),
                planes(start, rows, across, norb),
                slab_spec,
            ] + [hbm] * len(held),
            out_specs=(planes(start, rows, pairs, across), full((pairs, norb))),
            scratch_shapes=[pltpu.VMEM((rows * (pairs + GAP), LANES), F32)],
            input_output_aliases={5: 0} if held else {},
            compiler_params=params,
            cost_estimate=pl.CostEstimate(
                flops=2 * size * cells * norb * pairs, bytes_accessed=16 * size * cells * norb, transcendentals=0
            ),
            name="term",
        )(ax, pair_live, psi, orbitals, back, *held)
        part = part + share
    whole = lambda x: lax.all_to_all(x, ("gz", "gy"), split_axis=0, concat_axis=0, tiled=True)
    shares = whole(part.reshape(owners, per_dev, norb))
    mine_sum = jnp.sum(shares, axis=0, keepdims=True)
    summed = whole(jnp.broadcast_to(mine_sum, shares.shape)).reshape(pairs, norb)
    inner = lax.dot_general(
        summed, sel.astype(F32), (((0,), (0,)), ((), ())), precision=lax.Precision.HIGHEST, preferred_element_type=F32
    )
    tiles = (inner / (float(B) ** 3 / 4.0)).astype(BF)

    return pl.pallas_call(
        gradient_kernel,
        grid=(depth,),
        out_shape=jax.ShapeDtypeStruct(orbitals.shape, F32),
        in_specs=[
            full((pairs, norb)),
            full((norb, norb)),
            planes(0, rows, across, norb),
            planes(0, rows, pairs, across),
        ],
        out_specs=planes(0, rows, across, norb),
        compiler_params=params,
        name="gradient",
    )(hot_first, tiles, orbitals, term)


def solution(mesh):
    return jax.shard_map(
        body,
        mesh=mesh,
        in_specs=(P("gz", "gy", None, None), P(), P(), P()),
        out_specs=P("gz", "gy", None, None),
        check_vma=False,
    )
```
